32 devices in a mesh: dp: 4 (over x, y), tp: 8 (over z, core).
Axes of the slice: x: 2, y: 2, z: 4, core: 2. Of those that a mesh axis runs over, the one named last changes fastest.
Arguments:
- x: bfloat16 [11264, 3072], P(('dp', 'tp')), parts along dimension 0
- w_gate: bfloat16 [3072, 24576], P(None, 'tp')
- w_up: bfloat16 [3072, 24576], P(None, 'tp')
- w_down: bfloat16 [24576, 3072], P('tp')
Outputs:
- output: bfloat16 [11264, 3072], P(('dp', 'tp')), parts along dimension 0
There are 4 independent parts. The reference program is written for one: setup_inputs(seed, part) draws one part's arguments, and reference() takes and returns one part's arrays. A program takes and returns all parts, laid end to end along the dimension named above; an argument that names none is the same for every part.
All inputs are finite; a program needn't handle non-finite values.
Results may differ from the reference program's by a relative error of at most 0.016.
Values are sent between devices in bfloat16 or wider.
A program may use at most 2 GiB of HBM per device.

```python
import jax
import jax.numpy as jnp

ROWS = 2816
D = 3072
FF = 24576


def setup_inputs(seed: int = 0, part: int = 0) -> dict:
    kx, kg, ku, kd = jax.random.split(jax.random.key(seed), 4)
    drawn = {
        "x": jax.random.normal(jax.random.fold_in(kx, part), (ROWS, D), jnp.float32),
        "w_gate": jax.random.normal(kg, (D, FF), jnp.float32) * D**-0.5,
        "w_up": jax.random.normal(ku, (D, FF), jnp.float32) * D**-0.5,
        "w_down": jax.random.normal(kd, (FF, D), jnp.float32) * FF**-0.5,
    }
    return {k: v.astype(jnp.bfloat16) for k, v in drawn.items()}


def reference(x, w_gate, w_up, w_down):
    gate = jnp.dot(x, w_gate, preferred_element_type=jnp.float32)
    up = jnp.dot(x, w_up, preferred_element_type=jnp.float32)
    hidden = (jax.nn.gelu(gate) * up).astype(jnp.bfloat16)
    return jnp.dot(hidden, w_down, preferred_element_type=jnp.float32).astype(jnp.bfloat16)
```

```python
import functools

import jax
import jax.numpy as jnp
from jax import lax
from jax.experimental import pallas as pl
from jax.experimental.pallas import tpu as pltpu
from jax.sharding import PartitionSpec as P

CHIPS = 4
SLOTS = 2 * CHIPS
TILES = 6
HALF = TILES // 2
DELAY = 1
LAST = 2 * (SLOTS - 1) + 1 + DELAY


def mirror(item):
    return 6 - item + 2 * lax.rem(item, 2)


def gather_item(line, unit):
    slot = lax.div(unit, 2)
    item = jnp.where(slot <= line, 2 * (line - slot), 2 * (slot - line) - 1)
    return (line <= CHIPS - 2) & (slot < 2 * line + 2), item, lax.rem(unit, 2)


def sum_item(line, unit):
    slot = lax.div(unit - DELAY, 2)
    at, ahead = slot - (2 * line + 2), CHIPS - 1 - line
    item = jnp.where(at < ahead, 2 * (line + 1 + at), 2 * (CHIPS - 1 - (at - ahead)) + 1)
    valid = (line <= CHIPS - 2) & (at >= 0) & (slot < SLOTS)
    return valid, item, lax.rem(unit - DELAY, 2)


def kernel(
    x, wg, wu, wd, y, xg, stash, part, from_left, from_right,
    xv, hv, wgv, wuv, wdv, pst, sst, c_own, c_part, c_up, c_out,
    x_sem, w_sem, wd_sem, first_sem, ag_recv, d2d_recv, d2d_send, send, part_send, part_recv,
    stash_sem, load_sem, sum_recv, y_local, y_send, y_recv,
):
    rows, depth = x.shape
    ft, nt = wg.shape[1] // TILES, wd.shape[1] // TILES
    quarter, half_rows = rows // 4, rows // 2
    me = lax.axis_index("tp")
    z, c = lax.div(me, 2), lax.rem(me, 2)
    partner = me + 1 - 2 * c
    own, other = me, partner
    lines = (z, CHIPS - 1 - z)
    sources = (z - 1, CHIPS - 2 - z)
    targets = (me + 2, me - 2)
    sums = (from_left, from_right)

    def oriented(d, item):
        return item if d == 0 else mirror(item)

    def remote(src, dst, ssem, rsem, device):
        return pltpu.make_async_remote_copy(
            src_ref=src, dst_ref=dst, send_sem=ssem, recv_sem=rsem,
            device_id={"tp": device}, device_id_type=pl.DeviceIdType.MESH,
        )

    def rows_of(half, core):
        return pl.ds(pl.multiple_of((2 * half + core) * quarter, 8), quarter)

    def chunk(half):
        return pl.ds(pl.multiple_of(half * half_rows, 16), half_rows)

    def columns(i, size):
        return pl.ds(pl.multiple_of(i * size, size), size)

    def gather_copy(d, item, half, unit, src):
        return remote(src, xg.at[item, rows_of(half, c)], send.at[d, lax.rem(unit, 2)], ag_recv.at[item, half], targets[d])

    def start_gather(d, item, half, unit):
        @pl.when(item == own)
        def _():
            gather_copy(d, item, half, unit, x.at[rows_of(half, c)]).start()

        @pl.when(item != own)
        def _():
            gather_copy(d, item, half, unit, xg.at[item, rows_of(half, c)]).start()

    def wait_gathered(item, half):
        gather_copy(0, item, half, 0, xg.at[item, rows_of(half, c)]).wait_recv()

    def pass_on(d, item, half, unit, core):
        at = xg.at[item, rows_of(half, core)]
        return remote(at, at, d2d_send.at[d, lax.rem(unit, 2)], d2d_recv.at[item, half], partner)

    def sends(d, unit):
        a, _, _ = gather_item(lines[d], unit)
        b, _, _ = sum_item(lines[d], unit)
        return a | b

    def gather_service(v):
        for d in range(2):
            valid, item, half = gather_item(sources[d], v - 2)
            item = oriented(d, item)

            @pl.when(valid & (v >= 2))
            def _():
                pass_on(d, item, half, v - 2, c).wait_send()

            valid, item, half = gather_item(sources[d], v - 1)
            item = oriented(d, item)

            @pl.when(valid)
            def _():
                wait_gathered(item, half)
                pass_on(d, item, half, v - 1, c).start()

        for d in range(2):

            @pl.when(sends(d, v - 1))
            def _():
                gather_copy(d, own, 0, v - 1, xg.at[own, rows_of(0, c)]).wait_send()

            valid, item, half = gather_item(lines[d], v + 1)
            item = oriented(d, item)

            @pl.when(valid)
            def _():
                start_gather(d, item, half, v + 1)

    def loads(d, item, half, slot, n_up, ups):
        pairs = [(stash.at[item, :, chunk(half)], c_own.at[slot]), (part.at[item, :, chunk(half)], c_part.at[slot])]
        pairs += [(sums[up].at[item, :, chunk(half)], c_up.at[slot, up]) for up in ups]
        return [pltpu.make_async_copy(a, b, load_sem.at[slot, i]) for i, (a, b) in enumerate(pairs)]

    def part_copy(item, device, t, sem):
        return remote(pst.at[t], part.at[item, t], sem, part_recv.at[item], device)

    def wait_part(item):
        remote(part.at[item], part.at[item], part_send.at[0], part_recv.at[item], partner).wait_recv()

    def sum_copy(d, item, half, unit):
        return remote(
            c_out.at[d, lax.rem(unit, 2)], sums[d].at[item, :, chunk(half)],
            send.at[d, lax.rem(unit, 2)], sum_recv.at[d, item, half], targets[d],
        )

    def add(slot, out_slot, ups):
        @pl.loop(0, half_rows // 16)
        def _(i):
            at = pl.ds(pl.multiple_of(i * 16, 16), 16)
            total = c_own[slot, :, at, :] + c_part[slot, :, at, :].astype(jnp.float32)
            for up in ups:
                total += c_up[slot, up, :, at, :].astype(jnp.float32)
            c_out[slot, out_slot, :, at, :] = total.astype(jnp.bfloat16)

    def sum_cases(d, v, act):
        valid, item, half = sum_item(lines[d], v + 1)
        item = oriented(d, item)

        @pl.when(valid & (lines[d] == 0))
        def _():
            act(item, half, ())

        @pl.when(valid & (lines[d] > 0))
        def _():
            act(item, half, (d,))

    def sum_load(v):
        for d in range(2):

            def act(item, half, ups, d=d):
                @pl.when(half == 0)
                def _():
                    wait_part(item)

                for up in ups:
                    sum_copy(up, item, half, 0).wait_recv()
                for copy in loads(d, item, half, d, 0, ups):
                    copy.start()

            sum_cases(d, v, act)

    def sum_send(v):
        for d in range(2):

            def act(item, half, ups, d=d):
                for copy in loads(d, item, half, d, 0, ups):
                    copy.wait()
                add(d, lax.rem(v + 1, 2), ups)
                sum_copy(d, item, half, v + 1).start()

            sum_cases(d, v, act)

    def item_of(k):
        line = jnp.where(z < 2, z, CHIPS - 1 - z)
        item = jnp.int32(0)
        for i, (a, b) in enumerate(zip((2, 4, 6, 7, 5, 3), (4, 6, 0, 7, 1, 5))):
            item = jnp.where(k == i + 1, jnp.where(line == 0, a, b), item)
        item = jnp.where(z < 2, item, mirror(item))
        return jnp.where(k == 0, own, jnp.where(k == SLOTS - 1, other, item))

    def x_copy(item):
        return pltpu.make_async_copy(xg.at[item], xv, x_sem)

    def w_copies(i):
        return [
            pltpu.make_async_copy(w.at[:, columns(i, ft)], v.at[i], w_sem.at[n, i])
            for n, (w, v) in enumerate(((wg, wgv), (wu, wuv)))
        ]

    def column_tile(t):
        return jnp.where(t < HALF, (1 - c) * HALF + t, c * HALF + t - HALF)

    def wd_copy(t):
        slot = lax.rem(t, HALF)
        return pltpu.make_async_copy(wd.at[:, columns(column_tile(t), nt)], wdv.at[slot], wd_sem.at[slot])

    def stash_copy(item, t):
        return pltpu.make_async_copy(sst.at[t], stash.at[item, t], stash_sem.at[t])

    def wait_stored(item):
        for t in range(HALF):
            stash_copy(item, t).wait()
            part_copy(item, partner, t, part_send.at[t]).wait_send()

    barrier = pltpu.get_barrier_semaphore()

    def greet(device):
        pl.semaphore_signal(barrier, inc=1, device_id={"tp": device}, device_id_type=pl.DeviceIdType.MESH)

    greet(partner)
    for d in range(2):

        @pl.when(lines[d] <= CHIPS - 2)
        def _():
            greet(targets[d])

    pl.semaphore_wait(barrier, 1 + jnp.where(z > 0, 1, 0) + jnp.where(z < CHIPS - 1, 1, 0))

    def first_copy(n, half):
        at = rows_of(half, 1 - c if n == 0 else c)
        sem = (ag_recv if n == 0 else d2d_recv).at[own, half]
        return remote(x.at[at], xg.at[own, at], first_sem.at[n, half], sem, partner)

    def first_unit(unit):
        for d in range(2):

            @pl.when(lines[d] <= CHIPS - 2)
            def _():
                start_gather(d, 2 * z, unit, unit)

    for half in range(2):
        first_copy(0, half).start()

    @pl.when(c == 0)
    def _():
        first_unit(0)
        first_unit(1)

    for half in range(2):
        first_copy(1, half).start()
    pltpu.make_async_copy(x, xv, x_sem).start()

    @pl.loop(0, TILES)
    def _(i):
        for copy in w_copies(i):
            copy.start()

    for t in range(HALF):
        wd_copy(jnp.int32(t)).start()
    for half in range(2):
        wait_gathered(other, half)

        @pl.when(c == 1)
        def _():
            first_unit(half)

    pltpu.make_async_copy(x, xv, x_sem).wait()

    @pl.loop(0, SLOTS)
    def _(k):
        item, following = item_of(k), item_of(k + 1)

        @pl.when(k > 0)
        def _():
            x_copy(item).wait()
            wait_stored(item)

        @pl.loop(0, TILES)
        def _(i):
            @pl.when(k == 0)
            def _():
                for copy in w_copies(i):
                    copy.wait()

            @pl.when((i == 2))
            def _():
                gather_service(2 * k + 1)

            @pl.when((i == 0) | (i == 2))
            def _():
                sum_load(2 * k + lax.div(i, 2))

            @pl.when((i == 1) | (i == 3))
            def _():
                sum_send(2 * k + lax.div(i, 2))

            gate = jnp.dot(xv[...], wgv[i], preferred_element_type=jnp.float32)
            up = jnp.dot(xv[...], wuv[i], preferred_element_type=jnp.float32)
            hv[:, columns(i, ft)] = (jax.nn.gelu(gate) * up).astype(jnp.bfloat16)

        def down(t):
            wd_copy(t).wait()
            return jnp.dot(hv[...], wdv[lax.rem(t, HALF)], preferred_element_type=jnp.float32)

        @pl.loop(0, HALF)
        def _(t):
            @pl.when(t == 1)
            def _():
                gather_service(2 * k + 2)

            pst[t] = down(t).astype(jnp.bfloat16)
            part_copy(item, partner, t, part_send.at[t]).start()
            wd_copy(t + HALF).start()

        @pl.loop(0, HALF)
        def _(t):
            @pl.when((t == 1) & (k < SLOTS - 1))
            def _():
                for half in range(2):
                    pass_on(0, following, half, 0, 1 - c).wait_recv()
                x_copy(following).start()

            sst[t] = down(t + HALF)
            stash_copy(item, t).start()

            @pl.when(k < SLOTS - 1)
            def _():
                wd_copy(t).start()

    wait_stored(other)
    for d in range(2):

        @pl.when(sends(d, jnp.int32(LAST)))
        def _():
            gather_copy(d, own, 0, LAST, xg.at[own, rows_of(0, c)]).wait_send()

    for n in range(2):
        for half in range(2):
            first_copy(n, half).wait_send()

    def final_cases(act):
        @pl.when(z == 0)
        def _():
            act((1,))

        @pl.when((z > 0) & (z < CHIPS - 1))
        def _():
            act((0, 1))

        @pl.when(z == CHIPS - 1)
        def _():
            act((0,))

    def final_load(f):
        core, half = f // 2, f % 2
        if half == 0:
            wait_part(2 * z + core)

        def act(ups):
            for up in ups:
                sum_copy(up, 2 * z + core, half, 0).wait_recv()
            for copy in loads(f % 2, 2 * z + core, half, f % 2, 0, ups):
                copy.start()

        final_cases(act)

    def y_at(half, t):
        return y.at[chunk(half), columns(c * HALF + t, nt)]

    def final_store(f):
        core, half = f // 2, f % 2

        def act(ups):
            for copy in loads(f % 2, 2 * z + core, half, f % 2, 0, ups):
                copy.wait()
            add(f % 2, core, ups)

        final_cases(act)

        @pl.when(c == core)
        def _():
            for t in range(HALF):
                pltpu.make_async_copy(c_out.at[half, core, t], y_at(half, t), y_local.at[half, t]).start()

        @pl.when(c != core)
        def _():
            for t in range(HALF):
                y_copy(core, half, t).start()

    def y_copy(core, half, t):
        return remote(c_out.at[half, core, t], y_at(half, t), y_send.at[half, t], y_recv.at[half, t], partner)

    final_load(0)
    for f in range(4):
        if f < 3:
            final_load(f + 1)
        final_store(f)
    for half in range(2):
        for t in range(HALF):
            pltpu.make_async_copy(c_out.at[half, 0, t], y_at(half, t), y_local.at[half, t]).wait()
            y_copy(0, half, t).wait_send()
            y_copy(0, half, t).wait_recv()


def block(x, w_gate, w_up, w_down):
    rows, depth = x.shape
    width, out = w_gate.shape[1], w_down.shape[1]
    ft, nt = width // TILES, out // TILES
    bf16, f32 = jnp.bfloat16, jnp.float32
    half_rows = rows // 2
    shape = jax.ShapeDtypeStruct
    any_space = pl.BlockSpec(memory_space=pl.ANY)
    dma = pltpu.SemaphoreType.DMA
    results = pl.pallas_call(
        kernel,
        name="mlp_block",
        out_shape=[
            shape((rows, out), bf16),
            shape((SLOTS, rows, depth), bf16),
            shape((SLOTS, HALF, rows, nt), f32),
            shape((SLOTS, HALF, rows, nt), bf16),
            shape((SLOTS, HALF, rows, nt), bf16),
            shape((SLOTS, HALF, rows, nt), bf16),
        ],
        in_specs=[any_space] * 4,
        out_specs=[any_space] * 6,
        scratch_shapes=[
            pltpu.VMEM((rows, depth), bf16),
            pltpu.VMEM((rows, width), bf16),
            pltpu.VMEM((TILES, depth, ft), bf16),
            pltpu.VMEM((TILES, depth, ft), bf16),
            pltpu.VMEM((HALF, width, nt), bf16),
            pltpu.VMEM((HALF, rows, nt), bf16),
            pltpu.VMEM((HALF, rows, nt), f32),
            pltpu.VMEM((2, HALF, half_rows, nt), f32),
            pltpu.VMEM((2, HALF, half_rows, nt), bf16),
            pltpu.VMEM((2, 2, HALF, half_rows, nt), bf16),
            pltpu.VMEM((2, 2, HALF, half_rows, nt), bf16),
            dma(()),
            dma((2, TILES)),
            dma((HALF,)),
            dma((2, 2)),
            dma((SLOTS, 2)),
            dma((SLOTS, 2)),
            dma((2, 2)),
            dma((2, 2)),
            dma((HALF,)),
            dma((SLOTS,)),
            dma((HALF,)),
            dma((2, 4)),
            dma((2, SLOTS, 2)),
            dma((2, HALF)),
            dma((2, HALF)),
            dma((2, HALF)),
        ],
        compiler_params=pltpu.CompilerParams(
            collective_id=0, has_side_effects=True, vmem_limit_bytes=67_043_328
        ),
    )(x, w_gate, w_up, w_down)
    return results[0]


def solution(mesh):
    return jax.shard_map(
        block,
        mesh=mesh,
        in_specs=(P(("dp", "tp"), None), P(None, "tp"), P(None, "tp"), P("tp", None)),
        out_specs=P(("dp", "tp"), None),
        check_vma=False,
    )
```

```python
import functools

import jax
import jax.numpy as jnp
from jax import lax
from jax.experimental import pallas as pl
from jax.experimental.pallas import tpu as pltpu
from jax.sharding import PartitionSpec as P

CHIPS = 4
SLOTS = 2 * CHIPS
TILES = 6
HALF = TILES // 2


def mirror(item):
    return 6 - item + 2 * lax.rem(item, 2)


def gather_item(line, unit):
    slot = lax.div(unit, 2)
    item = jnp.where(slot <= line, 2 * (line - slot), 2 * (slot - line) - 1)
    return (line <= CHIPS - 2) & (slot < 2 * line + 2), item, lax.rem(unit, 2)


def sum_item(line, slot):
    at, ahead = slot - (2 * line + 2), CHIPS - 1 - line
    item = jnp.where(at < ahead, 2 * (line + 1 + at), 2 * (CHIPS - 1 - (at - ahead)) + 1)
    return (line <= CHIPS - 2) & (at >= 0) & (slot < SLOTS), item


def kernel(
    x, wg, wu, wd, y, xg, stash, part, from_left, from_right,
    xv, hv, wgv, wuv, wdv, pst, sst, c_own, c_part, c_up, c_out,
    x_sem, w_sem, wd_sem, first_sem, ag_recv, d2d_recv, d2d_send, send, part_send, part_recv,
    stash_sem, load_sem, sum_send_sem, sum_recv, fin_sem, y_local, y_send, y_recv,
):
    rows, depth = x.shape
    ft, nt = wg.shape[1] // TILES, wd.shape[1] // TILES
    assert ft == nt
    quarter, half_rows = rows // 4, rows // 2
    me = lax.axis_index("tp")
    z, c = lax.div(me, 2), lax.rem(me, 2)
    partner = me + 1 - 2 * c
    own, other = me, partner
    lines = (z, CHIPS - 1 - z)
    sources = (z - 1, CHIPS - 2 - z)
    targets = (me + 2, me - 2)
    sums = (from_left, from_right)

    def oriented(d, item):
        return item if d == 0 else mirror(item)

    def remote(src, dst, ssem, rsem, device):
        return pltpu.make_async_remote_copy(
            src_ref=src, dst_ref=dst, send_sem=ssem, recv_sem=rsem,
            device_id={"tp": device}, device_id_type=pl.DeviceIdType.MESH,
        )

    def rows_of(half, core):
        return pl.ds(pl.multiple_of((2 * half + core) * quarter, 8), quarter)

    def columns(i, size):
        return pl.ds(pl.multiple_of(i * size, size), size)

    def gather_copy(d, item, half, src):
        return remote(src, xg.at[item, rows_of(half, c)], send.at[d, half], ag_recv.at[item, half], targets[d])

    def start_gather(d, item, half):
        @pl.when(item == own)
        def _():
            gather_copy(d, item, half, x.at[rows_of(half, c)]).start()

        @pl.when(item != own)
        def _():
            gather_copy(d, item, half, xg.at[item, rows_of(half, c)]).start()

    def wait_gathered(item, half):
        gather_copy(0, item, half, xg.at[item, rows_of(half, c)]).wait_recv()

    def pass_on(d, item, half, core):
        at = xg.at[item, rows_of(half, core)]
        return remote(at, at, d2d_send.at[d, half], d2d_recv.at[item, half], partner)

    def gather_service(v):
        for d in range(2):
            valid, item, half = gather_item(sources[d], v - 2)
            item = oriented(d, item)

            @pl.when(valid & (v >= 2))
            def _():
                pass_on(d, item, half, c).wait_send()

            valid, item, half = gather_item(sources[d], v - 1)
            item = oriented(d, item)

            @pl.when(valid)
            def _():
                wait_gathered(item, half)
                pass_on(d, item, half, c).start()

        for d in range(2):
            valid, item, half = gather_item(lines[d], v - 1)

            @pl.when(valid)
            def _():
                gather_copy(d, own, half, xg.at[own, rows_of(half, c)]).wait_send()

            valid, item, half = gather_item(lines[d], v + 1)
            item = oriented(d, item)

            @pl.when(valid)
            def _():
                start_gather(d, item, half)

    def loads(d, item, t, ups):
        pairs = [(stash.at[item, t], c_own.at[d]), (part.at[item, t], c_part.at[d])]
        pairs += [(sums[up].at[item, t], c_up.at[d]) for up in ups]
        return [pltpu.make_async_copy(a, b, load_sem.at[d, i]) for i, (a, b) in enumerate(pairs)]

    def part_copy(item, t):
        return remote(pst.at[t], part.at[item, t], part_send.at[t], part_recv.at[item, t], partner)

    def sum_copy(d, item, t):
        return remote(
            c_out.at[d, t], sums[d].at[item, t], sum_send_sem.at[d, t], sum_recv.at[d, item, t], targets[d]
        )

    def add(own_ref, others, out):
        step = rows // 11 if rows % 176 == 0 else 16

        @pl.loop(0, rows // step)
        def _(i):
            at = pl.ds(pl.multiple_of(i * step, 16), step)
            total = own_ref[at, :]
            for ref in others:
                total += ref[at, :].astype(jnp.float32)
            out[at, :] = total.astype(jnp.bfloat16)

    def sum_cases(d, slot, act):
        valid, item = sum_item(lines[d], slot)
        item = oriented(d, item)

        @pl.when(valid & (lines[d] == 0))
        def _():
            act(item, ())

        @pl.when(valid & (lines[d] > 0))
        def _():
            act(item, (d,))

    def stored(t):
        stash_copy(own, t).wait()
        part_copy(own, t).wait_send()

    def sum_load(slot, t):
        for d in range(2):

            def act(item, ups, d=d):
                part_copy(item, t).wait_recv()
                for up in ups:
                    sum_copy(up, item, t).wait_recv()
                for copy in loads(d, item, t, ups):
                    copy.start()

            sum_cases(d, slot, act)

    def sum_send(slot, t):
        for d in range(2):

            @pl.when(sum_item(lines[d], slot - 1)[0])
            def _():
                sum_copy(d, own, t).wait_send()

            def act(item, ups, d=d):
                for copy in loads(d, item, t, ups):
                    copy.wait()
                add(c_own.at[d], [c_part.at[d]] + [c_up.at[d] for _ in ups], c_out.at[d, t])
                sum_copy(d, item, t).start()

            sum_cases(d, slot, act)

    def item_of(k):
        line = jnp.where(z < 2, z, CHIPS - 1 - z)
        item = jnp.int32(0)
        for i, (a, b) in enumerate(zip((2, 4, 6, 7, 5, 3), (4, 6, 0, 7, 1, 5))):
            item = jnp.where(k == i + 1, jnp.where(line == 0, a, b), item)
        item = jnp.where(z < 2, item, mirror(item))
        return jnp.where(k == 0, own, jnp.where(k == SLOTS - 1, other, item))

    def x_copy(item, half):
        at = pl.ds(half * half_rows, half_rows)
        return pltpu.make_async_copy(xg.at[item, at], xv.at[at], x_sem.at[half])

    def x_load(item, half):
        pass_on(0, item, half, 1 - c).wait_recv()
        x_copy(item, half).start()

    def w_copies(i):
        return [
            pltpu.make_async_copy(w.at[:, columns(i, ft)], v.at[i], w_sem.at[n, i])
            for n, (w, v) in enumerate(((wg, wgv), (wu, wuv)))
        ]

    def wd_copies(pair):
        t, base = lax.rem(pair, HALF), 2 * lax.rem(pair, 2)
        return [
            pltpu.make_async_copy(
                wd.at[:, columns(core * HALF + t, nt)], wdv.at[base + j], wd_sem.at[base + j]
            )
            for j, core in enumerate((c, 1 - c))
        ]

    def stash_copy(item, t):
        return pltpu.make_async_copy(sst.at[t], stash.at[item, t], stash_sem.at[t])

    x_first = pltpu.make_async_copy(x, xv, x_sem.at[0])
    x_first.start()
    for copy in w_copies(0):
        copy.start()
    barrier = pltpu.get_barrier_semaphore()

    def greet(device):
        pl.semaphore_signal(barrier, inc=1, device_id={"tp": device}, device_id_type=pl.DeviceIdType.MESH)

    greet(partner)
    for d in range(2):

        @pl.when(lines[d] <= CHIPS - 2)
        def _():
            greet(targets[d])

    pl.semaphore_wait(barrier, 1 + jnp.where(z > 0, 1, 0) + jnp.where(z < CHIPS - 1, 1, 0))

    def first_copy(n, half):
        at = rows_of(half, 1 - c if n == 0 else c)
        sem = (ag_recv if n == 0 else d2d_recv).at[own, half]
        return remote(x.at[at], xg.at[own, at], first_sem.at[n, half], sem, partner)

    def first_unit(unit):
        for d in range(2):

            @pl.when(lines[d] <= CHIPS - 2)
            def _():
                start_gather(d, 2 * z, unit)

    for half in range(2):
        first_copy(0, half).start()

    @pl.when(c == 0)
    def _():
        first_unit(0)
        first_unit(1)

    for half in range(2):
        first_copy(1, half).start()

    @pl.loop(1, TILES)
    def _(i):
        for copy in w_copies(i):
            copy.start()

    for pair in range(2):
        for copy in wd_copies(jnp.int32(pair)):
            copy.start()
    for half in range(2):
        wait_gathered(other, half)

        @pl.when(c == 1)
        def _():
            first_unit(half)

    x_first.wait()

    spare = pl.ds(0, rows)

    def final_cases(act):
        @pl.when(z == 0)
        def _():
            act((1,))

        @pl.when((z > 0) & (z < CHIPS - 1))
        def _():
            act((0, 1))

        @pl.when(z == CHIPS - 1)
        def _():
            act((0,))

    def part_in(item, t):
        n = lax.rem(item, 2) * HALF + t
        return pltpu.make_async_copy(part.at[item, t], wgv.at[n, spare], fin_sem.at[n, 0])

    def part_load(item, t):
        part_copy(item, t).wait_recv()
        part_in(item, t).start()

    def own_load(t):
        return pltpu.make_async_copy(stash.at[own, t], c_own.at[t], fin_sem.at[t, 3])

    def up_in(core, t, up):
        n = core * HALF + t
        return pltpu.make_async_copy(
            sums[up].at[2 * z + core, t], wuv.at[n, pl.ds(up * rows, rows)], fin_sem.at[n, 1 + up]
        )

    def up_load(core, t):
        def act(ups):
            for up in ups:
                sum_copy(up, 2 * z + core, t).wait_recv()
                up_in(core, t, up).start()

        final_cases(act)

    def final_early():
        for t in range(HALF):
            own_load(t).start()
            part_load(other, t)
            up_load(0, t)

    def staged(core, t):
        return hv.at[:, columns(core * HALF + t, nt)]

    def y_at(t):
        return y.at[:, columns(c * HALF + t, nt)]

    def y_stay(core, t):
        return pltpu.make_async_copy(staged(core, t), y_at(t), y_local.at[t])

    def y_leave(core, t):
        return remote(staged(core, t), y_at(t), y_send.at[t], y_recv.at[t], partner)

    def final_store(core, t):
        n = core * HALF + t

        def act(ups):
            part_in(2 * z + core, t).wait()
            for up in ups:
                up_in(core, t, up).wait()
            others = [wgv.at[n, spare]] + [wuv.at[n, pl.ds(up * rows, rows)] for up in ups]

            @pl.when(c == core)
            def _():
                own_load(t).wait()
                add(c_own.at[t], others, staged(core, t))
                y_stay(core, t).start()

            @pl.when(c != core)
            def _():
                add(sst.at[t], others, staged(core, t))
                y_leave(core, t).start()

        final_cases(act)

    @pl.loop(0, SLOTS)
    def _(k):
        item, following = item_of(k), item_of(k + 1)

        def gate_up(n, at):
            gate = jnp.dot(xv[at, :], wgv[n], preferred_element_type=jnp.float32)
            up = jnp.dot(xv[at, :], wuv[n], preferred_element_type=jnp.float32)
            hv[at, columns(n, ft)] = (jax.nn.gelu(gate) * up).astype(jnp.bfloat16)

        def prefetch(t):
            for copy in wd_copies(HALF * k + t):
                copy.start()

        @pl.when(k == 0)
        def _():
            @pl.loop(0, HALF)
            def _(i):
                for j in range(2):
                    for copy in w_copies(2 * i + j):
                        copy.wait()
                for j in range(2):
                    gate_up(2 * i + j, pl.ds(0, rows))

        @pl.when(k > 0)
        def _():
            sum_send(k, 0)
            stored(1)
            sum_load(k, 1)
            x_copy(item, 0).wait()

            @pl.loop(0, TILES)
            def _(i):
                half = lax.div(i, HALF)

                @pl.when(i == 1)
                def _():
                    gather_service(2 * k)

                @pl.when((i == 1) | (i == 3))
                def _():
                    sum_send(k, lax.div(i + 1, 2))

                @pl.when(i == 2)
                def _():
                    stored(2)
                    sum_load(k, 2)
                    x_load(item, 1)

                @pl.when(i == HALF)
                def _():
                    x_copy(item, 1).wait()

                @pl.when((i == HALF) | (i == HALF + 1))
                def _():
                    prefetch(i - HALF)

                for j in range(2):
                    at = pl.ds(pl.multiple_of(half * half_rows, 16), half_rows)
                    gate_up(2 * lax.rem(i, HALF) + j, at)

        @pl.loop(0, HALF)
        def _(t):
            @pl.when(t == 0)
            def _():
                gather_service(2 * k + 1)

            @pl.when((k < SLOTS - 1) & (t == jnp.where(k == 0, 1, 2)))
            def _():
                x_load(following, 0)

            @pl.when(t == 2)
            def _():
                stored(0)
                sum_load(k + 1, 0)

            @pl.when((k == SLOTS - 1) & (t == 0))
            def _():
                final_early()

            @pl.when((k == SLOTS - 1) & (t == 2))
            def _():
                part_load(own, 0)

            pair = HALF * k + t
            base = 2 * lax.rem(pair, 2)
            for copy in wd_copies(pair):
                copy.wait()
            mine = jnp.dot(hv[...], wdv[base], preferred_element_type=jnp.float32)
            theirs = jnp.dot(hv[...], wdv[base + 1], preferred_element_type=jnp.float32)
            sst[t] = mine
            pst[t] = theirs.astype(jnp.bfloat16)
            stash_copy(item, t).start()
            part_copy(item, t).start()

            @pl.when(t == 0)
            def _():
                prefetch(2)

    part_load(own, 1)
    up_load(1, 0)
    part_load(own, 2)
    up_load(1, 1)
    for t in range(HALF):
        final_store(0, t)
    final_store(1, 0)
    up_load(1, 2)
    final_store(1, 1)
    final_store(1, 2)
    for t in range(1, HALF):
        stored(t)
    for d in range(2):

        @pl.when(lines[d] <= CHIPS - 2)
        def _():
            for t in range(HALF):
                sum_copy(d, own, t).wait_send()

    for n in range(2):
        for half in range(2):
            first_copy(n, half).wait_send()
    for t in range(HALF):
        y_stay(0, t).wait()
        y_leave(0, t).wait_send()
        y_leave(0, t).wait_recv()


def block(x, w_gate, w_up, w_down):
    rows, depth = x.shape
    width, out = w_gate.shape[1], w_down.shape[1]
    ft, nt = width // TILES, out // TILES
    bf16, f32 = jnp.bfloat16, jnp.float32
    shape = jax.ShapeDtypeStruct
    any_space = pl.BlockSpec(memory_space=pl.ANY)
    dma = pltpu.SemaphoreType.DMA
    results = pl.pallas_call(
        kernel,
        name="mlp_block",
        out_shape=[
            shape((rows, out), bf16),
            shape((SLOTS, rows, depth), bf16),
            shape((SLOTS, HALF, rows, nt), f32),
            shape((SLOTS, HALF, rows, nt), bf16),
            shape((SLOTS, HALF, rows, nt), bf16),
            shape((SLOTS, HALF, rows, nt), bf16),
        ],
        in_specs=[any_space] * 4,
        out_specs=[any_space] * 6,
        scratch_shapes=[
            pltpu.VMEM((rows, depth), bf16),
            pltpu.VMEM((rows, width), bf16),
            pltpu.VMEM((TILES, depth, ft), bf16),
            pltpu.VMEM((TILES, depth, ft), bf16),
            pltpu.VMEM((4, width, nt), bf16),
            pltpu.VMEM((HALF, rows, nt), bf16),
            pltpu.VMEM((HALF, rows, nt), f32),
            pltpu.VMEM((HALF, rows, nt), f32),
            pltpu.VMEM((2, rows, nt), bf16),
            pltpu.VMEM((2, rows, nt), bf16),
            pltpu.VMEM((2, HALF, rows, nt), bf16),
            dma((2,)),
            dma((2, TILES)),
            dma((4,)),
            dma((2, 2)),
            dma((SLOTS, 2)),
            dma((SLOTS, 2)),
            dma((2, 2)),
            dma((2, 2)),
            dma((HALF,)),
            dma((SLOTS, HALF)),
            dma((HALF,)),
            dma((2, 3)),
            dma((2, HALF)),
            dma((2, SLOTS, HALF)),
            dma((TILES, 4)),
            dma((HALF,)),
            dma((HALF,)),
            dma((HALF,)),
        ],
        compiler_params=pltpu.CompilerParams(
            collective_id=0, has_side_effects=True, vmem_limit_bytes=67_043_328
        ),
    )(x, w_gate, w_up, w_down)
    return results[0]


def solution(mesh):
    return jax.shard_map(
        block,
        mesh=mesh,
        in_specs=(P(("dp", "tp"), None), P(None, "tp"), P(None, "tp"), P("tp", None)),
        out_specs=P(("dp", "tp"), None),
        check_vma=False,
    )
```

```python
import functools

import jax
import jax.numpy as jnp
from jax import lax
from jax.experimental import pallas as pl
from jax.experimental.pallas import tpu as pltpu
from jax.sharding import PartitionSpec as P

CHIPS = 4
SLOTS = 2 * CHIPS
TILES = 6
HALF = TILES // 2


def mirror(item):
    return 6 - item + 2 * lax.rem(item, 2)


def gather_item(line, unit):
    slot = lax.div(unit, 2)
    item = jnp.where(slot <= line, 2 * (line - slot), 2 * (slot - line) - 1)
    return (line <= CHIPS - 2) & (slot < 2 * line + 2), item, lax.rem(unit, 2)


def sum_item(line, slot):
    at, ahead = slot - (2 * line + 2), CHIPS - 1 - line
    item = jnp.where(at < ahead, 2 * (line + 1 + at), 2 * (CHIPS - 1 - (at - ahead)) + 1)
    return (line <= CHIPS - 2) & (at >= 0) & (slot < SLOTS), item


def kernel(
    x, wg, wu, wd, y, xg, stash, part, from_left, from_right,
    xv, hv, wgv, wuv, wdv, pst, sst, c_own, c_part, c_up, c_out,
    x_sem, w_sem, wd_sem, first_sem, ag_recv, d2d_recv, d2d_send, send, part_send, part_recv,
    stash_sem, load_sem, sum_send_sem, sum_recv, y_sem,
):
    rows, depth = x.shape
    ft, nt = wg.shape[1] // TILES, wd.shape[1] // TILES
    assert ft == nt
    quarter, half_rows = rows // 4, rows // 2
    me = lax.axis_index("tp")
    z, c = lax.div(me, 2), lax.rem(me, 2)
    partner = me + 1 - 2 * c
    own, other = me, partner
    lines = (z, CHIPS - 1 - z)
    sources = (z - 1, CHIPS - 2 - z)
    targets = (me + 2, me - 2)
    sums = (from_left, from_right)

    def oriented(d, item):
        return item if d == 0 else mirror(item)

    def remote(src, dst, ssem, rsem, device):
        return pltpu.make_async_remote_copy(
            src_ref=src, dst_ref=dst, send_sem=ssem, recv_sem=rsem,
            device_id={"tp": device}, device_id_type=pl.DeviceIdType.MESH,
        )

    def rows_of(half, core):
        return pl.ds(pl.multiple_of((2 * half + core) * quarter, 8), quarter)

    def columns(i, size):
        return pl.ds(pl.multiple_of(i * size, size), size)

    def gather_copy(d, item, half, src):
        return remote(src, xg.at[item, rows_of(half, c)], send.at[d, half], ag_recv.at[item, half], targets[d])

    def start_gather(d, item, half):
        @pl.when(item == own)
        def _():
            gather_copy(d, item, half, x.at[rows_of(half, c)]).start()

        @pl.when(item != own)
        def _():
            gather_copy(d, item, half, xg.at[item, rows_of(half, c)]).start()

    def wait_gathered(item, half):
        gather_copy(0, item, half, xg.at[item, rows_of(half, c)]).wait_recv()

    def pass_on(d, item, half, core):
        at = xg.at[item, rows_of(half, core)]
        return remote(at, at, d2d_send.at[d, half], d2d_recv.at[item, half], partner)

    def gather_service(v):
        for d in range(2):
            valid, item, half = gather_item(sources[d], v - 2)
            item = oriented(d, item)

            @pl.when(valid & (v >= 2))
            def _():
                pass_on(d, item, half, c).wait_send()

            valid, item, half = gather_item(sources[d], v - 1)
            item = oriented(d, item)

            @pl.when(valid)
            def _():
                wait_gathered(item, half)
                pass_on(d, item, half, c).start()

        for d in range(2):
            valid, item, half = gather_item(lines[d], v - 1)

            @pl.when(valid)
            def _():
                gather_copy(d, own, half, xg.at[own, rows_of(half, c)]).wait_send()

            valid, item, half = gather_item(lines[d], v + 1)
            item = oriented(d, item)

            @pl.when(valid)
            def _():
                start_gather(d, item, half)

    def loads(d, item, t, ups):
        pairs = [(stash.at[item, t], c_own.at[d]), (part.at[item, t], c_part.at[d])]
        pairs += [(sums[up].at[item, t], c_up.at[d]) for up in ups]
        return [pltpu.make_async_copy(a, b, load_sem.at[d, i]) for i, (a, b) in enumerate(pairs)]

    def part_copy(item, t):
        return remote(pst.at[t], part.at[item, t], part_send.at[0, t], part_recv.at[item, t], partner)

    def part_rest(t):
        at = xv.at[:, columns(t, nt)]
        return remote(at, part.at[me, t], part_send.at[1, t], part_recv.at[me, t], partner)

    def sum_sem(d, chip, index, t):
        both = lax.div(index, 2) == chip
        return sum_recv.at[jnp.where(both & (d == 1), SLOTS + lax.rem(index, 2), index), t]

    def sum_copy(d, item, t):
        ends = lax.div(item, 2) == lax.div(targets[d], 2)
        index, device = jnp.where(ends, targets[d], item), jnp.where(ends, item, targets[d])
        return remote(
            c_out.at[d, t], sums[d].at[index, t], sum_send_sem.at[d, t],
            sum_sem(d, lax.div(targets[d], 2), index, t), device,
        )

    def wait_sum(d, index, t):
        at = sums[d].at[index, t]
        remote(at, at, sum_send_sem.at[d, t], sum_sem(d, z, index, t), partner).wait_recv()

    def add(own_ref, others, out):
        step = rows // 11 if rows % 176 == 0 else 16

        @pl.loop(0, rows // step)
        def _(i):
            at = pl.ds(pl.multiple_of(i * step, 16), step)
            total = own_ref[at, :]
            for ref in others:
                total += ref[at, :].astype(jnp.float32)
            out[at, :] = total.astype(jnp.bfloat16)

    def sum_cases(d, slot, act):
        valid, item = sum_item(lines[d], slot)
        item = oriented(d, item)

        @pl.when(valid & (lines[d] == 0))
        def _():
            act(item, ())

        @pl.when(valid & (lines[d] > 0))
        def _():
            act(item, (d,))

    def stored(slot, t):
        stash_copy(own, t).wait()

        @pl.when(slot == 0)
        def _():
            stash_rest(t).wait()

        @pl.when(slot > 0)
        def _():
            part_copy(own, t).wait_send()


    def sum_load(slot, t):
        for d in range(2):

            def act(item, ups, d=d):
                part_copy(item, t).wait_recv()
                for up in ups:
                    wait_sum(up, item, t)
                for copy in loads(d, item, t, ups):
                    copy.start()

            sum_cases(d, slot, act)

    def sum_send(slot, t):
        for d in range(2):

            @pl.when(sum_item(lines[d], slot - 1)[0])
            def _():
                sum_copy(d, own, t).wait_send()

            def act(item, ups, d=d):
                for copy in loads(d, item, t, ups):
                    copy.wait()
                add(c_own.at[d], [c_part.at[d]] + [c_up.at[d] for _ in ups], c_out.at[d, t])
                sum_copy(d, item, t).start()

            sum_cases(d, slot, act)

    def item_of(k):
        line = jnp.where(z < 2, z, CHIPS - 1 - z)
        item = jnp.int32(0)
        for i, (a, b) in enumerate(zip((2, 4, 6, 7, 5, 3), (4, 6, 0, 7, 1, 5))):
            item = jnp.where(k == i + 1, jnp.where(line == 0, a, b), item)
        item = jnp.where(z < 2, item, mirror(item))
        return jnp.where(k == 0, own, jnp.where(k == SLOTS - 1, other, item))

    def x_copy(item, half):
        at = pl.ds(half * half_rows, half_rows)
        return pltpu.make_async_copy(xg.at[item, at], xv.at[at], x_sem.at[half])

    def x_load(item, half):
        pass_on(0, item, half, 1 - c).wait_recv()
        x_copy(item, half).start()

    def w_copies(i):
        return [
            pltpu.make_async_copy(w.at[:, columns(i, ft)], v.at[i], w_sem.at[n, i])
            for n, (w, v) in enumerate(((wg, wgv), (wu, wuv)))
        ]

    def wd_copies(pair):
        t, base = lax.rem(pair, HALF), 2 * lax.rem(pair, 2)
        return [
            pltpu.make_async_copy(
                wd.at[:, columns(core * HALF + t, nt)], wdv.at[base + j], wd_sem.at[base + j]
            )
            for j, core in enumerate((c, 1 - c))
        ]

    def stash_copy(item, t):
        return pltpu.make_async_copy(sst.at[t], stash.at[item, t], stash_sem.at[0, t])

    def stash_rest(t):
        return pltpu.make_async_copy(c_own.at[t], stash.at[other, t], stash_sem.at[1, t])

    x_first = pltpu.make_async_copy(x, xv, x_sem.at[0])
    x_first.start()
    for copy in w_copies(0):
        copy.start()
    barrier = pltpu.get_barrier_semaphore()

    def greet(device):
        pl.semaphore_signal(barrier, inc=1, device_id={"tp": device}, device_id_type=pl.DeviceIdType.MESH)

    greet(partner)
    for d in range(2):

        @pl.when(lines[d] <= CHIPS - 2)
        def _():
            greet(targets[d])
            greet(targets[d] + 1 - 2 * c)

    pl.semaphore_wait(barrier, 1 + jnp.where(z > 0, 2, 0) + jnp.where(z < CHIPS - 1, 2, 0))

    def first_copy(n, half):
        at = rows_of(half, 1 - c if n == 0 else c)
        sem = (ag_recv if n == 0 else d2d_recv).at[own, half]
        return remote(x.at[at], xg.at[own, at], first_sem.at[n, half], sem, partner)

    def first_unit(unit):
        for d in range(2):

            @pl.when(lines[d] <= CHIPS - 2)
            def _():
                start_gather(d, 2 * z, unit)

    for half in range(2):
        first_copy(0, half).start()

    @pl.when(c == 0)
    def _():
        first_unit(0)
        first_unit(1)

    for half in range(2):
        first_copy(1, half).start()

    @pl.loop(1, TILES)
    def _(i):
        for copy in w_copies(i):
            copy.start()

    for pair in range(2):
        for copy in wd_copies(jnp.int32(pair)):
            copy.start()
    for half in range(2):
        wait_gathered(other, half)

        @pl.when(c == 1)
        def _():
            first_unit(half)

    x_first.wait()

    spare = pl.ds(0, rows)

    def final_cases(act):
        @pl.when(z == 0)
        def _():
            act((1,))

        @pl.when((z > 0) & (z < CHIPS - 1))
        def _():
            act((0, 1))

        @pl.when(z == CHIPS - 1)
        def _():
            act((0,))

    def own_ref(h, t):
        return c_own.at[t] if h == 0 else sst.at[t]

    def final_copy(h, t, i):
        n, index = h * HALF + t, 2 * z + h
        if i == 0:
            src, dst = stash.at[index, t], own_ref(h, t)
        elif i == 1:
            src, dst = part.at[index, t], wgv.at[n, spare]
        else:
            src, dst = sums[i - 2].at[index, t], wuv.at[n, pl.ds((i - 2) * rows, rows)]
        sem = (
            w_sem.at[0, n],
            w_sem.at[1, n],
            load_sem.at[h, t],
            d2d_send.at[h, t] if t < HALF - 1 else x_sem.at[h],
        )[i]
        return pltpu.make_async_copy(src, dst, sem)

    def part_load(t, rest):
        for h in range(2):

            @pl.when((h == c) == (rest == 0))
            def _():
                part_copy(2 * z + h, t).wait_recv()
                final_copy(h, t, 1).start()

    def up_load(t):
        def act(ups):
            for h in range(2):
                for up in ups:
                    wait_sum(up, 2 * z + h, t)
                    final_copy(h, t, 2 + up).start()

        final_cases(act)

    def y_copy(h, t):
        return pltpu.make_async_copy(
            hv.at[:, columns(h * HALF + t, nt)], y.at[:, columns(h * HALF + t, nt)], y_sem
        )

    def final_store(t):
        def act(ups):
            for h in range(2):
                n = h * HALF + t
                for i in (0, 1, *(2 + up for up in ups)):
                    final_copy(h, t, i).wait()
                others = [wgv.at[n, spare]] + [wuv.at[n, pl.ds(up * rows, rows)] for up in ups]
                add(own_ref(h, t), others, hv.at[:, columns(n, nt)])
                y_copy(h, t).start()

        final_cases(act)

    @pl.loop(0, SLOTS)
    def _(k):
        item, following = item_of(k), item_of(k + 1)

        def gate_up(n, at):
            gate = jnp.dot(xv[at, :], wgv[n], preferred_element_type=jnp.float32)
            up = jnp.dot(xv[at, :], wuv[n], preferred_element_type=jnp.float32)
            hv[at, columns(n, ft)] = (jax.nn.gelu(gate) * up).astype(jnp.bfloat16)

        def prefetch(t):
            for copy in wd_copies(HALF * k + t):
                copy.start()

        @pl.when(k == 0)
        def _():
            @pl.loop(0, HALF)
            def _(i):
                for j in range(2):
                    for copy in w_copies(2 * i + j):
                        copy.wait()
                for j in range(2):
                    gate_up(2 * i + j, pl.ds(0, rows))

        @pl.when(k > 0)
        def _():
            sum_send(k, 0)
            stored(k - 1, 1)
            sum_load(k, 1)
            x_copy(item, 0).wait()

            upper, lower = (pl.ds(half * half_rows, half_rows) for half in range(2))
            for n in range(2):
                gate_up(n, upper)
            gather_service(2 * k)
            sum_send(k, 1)
            for n in range(2, 4):
                gate_up(n, upper)
            x_load(item, 1)
            for n in range(4, TILES):
                gate_up(n, upper)
            stored(k - 1, 2)
            sum_load(k, 2)
            x_copy(item, 1).wait()
            prefetch(0)
            for n in range(2):
                gate_up(n, lower)
            sum_send(k, 2)
            prefetch(1)
            for n in range(2, TILES):
                gate_up(n, lower)

        def down(pair):
            base = 2 * lax.rem(pair, 2)
            for copy in wd_copies(pair):
                copy.wait()
            return tuple(
                jnp.dot(hv[...], wdv[base + j], preferred_element_type=jnp.float32) for j in range(2)
            )

        @pl.when(k == 0)
        def _():
            @pl.loop(0, HALF)
            def _(t):
                @pl.when(t == 0)
                def _():
                    gather_service(1)

                @pl.when(t == 1)
                def _():
                    x_load(following, 0)

                @pl.when(t == 2)
                def _():
                    stored(0, 0)

                mine, theirs = down(t)
                sst[t] = mine
                c_own[t] = theirs
                stash_copy(own, t).start()
                stash_rest(t).start()

                @pl.when(t == 0)
                def _():
                    prefetch(2)

        @pl.when(k > 0)
        def _():
            kept = jnp.where(k < SLOTS - 1, item, SLOTS)

            def tile_pair(t):
                mine, theirs = down(HALF * k + t)
                sst[t] = mine
                pst[t] = theirs.astype(jnp.bfloat16)
                stash_copy(kept, t).start()
                part_copy(item, t).start()

            def send_rest(t):
                add(sst.at[t], [], xv.at[:, columns(t, nt)])
                part_rest(t).start()

            gather_service(2 * k + 1)

            @pl.when(k == SLOTS - 1)
            def _():
                for n in range(HALF):
                    final_copy(0, n, 0).start()
                up_load(0)

            tile_pair(0)
            prefetch(2)
            tile_pair(1)

            @pl.when(k < SLOTS - 1)
            def _():
                x_load(following, 0)

            stored(k, 0)
            sum_load(k + 1, 0)

            @pl.when(k == SLOTS - 1)
            def _():
                for t in range(2):
                    send_rest(t)
                final_copy(1, 0, 0).start()
                part_load(0, 0)
                up_load(1)

            tile_pair(2)

            @pl.when(k == SLOTS - 1)
            def _():
                send_rest(2)

    stored(jnp.int32(SLOTS - 1), 1)
    final_copy(1, 1, 0).start()
    part_load(0, 1)
    for t in range(1, HALF):
        for rest in range(2):
            part_load(t, rest)
    stored(jnp.int32(SLOTS - 1), 2)
    final_copy(1, 2, 0).start()
    final_store(0)
    final_store(1)
    up_load(2)
    final_store(2)
    for t in range(HALF):
        part_rest(t).wait_send()
    for d in range(2):

        @pl.when(lines[d] <= CHIPS - 2)
        def _():
            for t in range(HALF):
                sum_copy(d, own, t).wait_send()

    for n in range(2):
        for half in range(2):
            first_copy(n, half).wait_send()
    pltpu.make_async_copy(hv, y, y_sem).wait()


def block(x, w_gate, w_up, w_down):
    rows, depth = x.shape
    width, out = w_gate.shape[1], w_down.shape[1]
    ft, nt = width // TILES, out // TILES
    bf16, f32 = jnp.bfloat16, jnp.float32
    shape = jax.ShapeDtypeStruct
    any_space = pl.BlockSpec(memory_space=pl.ANY)
    dma = pltpu.SemaphoreType.DMA
    results = pl.pallas_call(
        kernel,
        name="mlp_block",
        out_shape=[
            shape((rows, out), bf16),
            shape((SLOTS, rows, depth), bf16),
            shape((SLOTS + 1, HALF, rows, nt), f32),
            shape((SLOTS, HALF, rows, nt), bf16),
            shape((SLOTS, HALF, rows, nt), bf16),
            shape((SLOTS, HALF, rows, nt), bf16),
        ],
        in_specs=[any_space] * 4,
        out_specs=[any_space] * 6,
        scratch_shapes=[
            pltpu.VMEM((rows, depth), bf16),
            pltpu.VMEM((rows, width), bf16),
            pltpu.VMEM((TILES, depth, ft), bf16),
            pltpu.VMEM((TILES, depth, ft), bf16),
            pltpu.VMEM((4, width, nt), bf16),
            pltpu.VMEM((HALF, rows, nt), bf16),
            pltpu.VMEM((HALF, rows, nt), f32),
            pltpu.VMEM((HALF, rows, nt), f32),
            pltpu.VMEM((2, rows, nt), bf16),
            pltpu.VMEM((2, rows, nt), bf16),
            pltpu.VMEM((2, HALF, rows, nt), bf16),
            dma((2,)),
            dma((2, TILES)),
            dma((4,)),
            dma((2, 2)),
            dma((SLOTS, 2)),
            dma((SLOTS, 2)),
            dma((2, 2)),
            dma((2, 2)),
            dma((2, HALF)),
            dma((SLOTS, HALF)),
            dma((2, HALF)),
            dma((2, 3)),
            dma((2, HALF)),
            dma((SLOTS + 2, HALF)),
            dma(()),
        ],
        compiler_params=pltpu.CompilerParams(
            collective_id=0, has_side_effects=True, vmem_limit_bytes=67_043_328
        ),
    )(x, w_gate, w_up, w_down)
    return results[0]


def solution(mesh):
    return jax.shard_map(
        block,
        mesh=mesh,
        in_specs=(P(("dp", "tp"), None), P(None, "tp"), P(None, "tp"), P("tp", None)),
        out_specs=P(("dp", "tp"), None),
        check_vma=False,
    )
```

```python
import functools

import jax
import jax.numpy as jnp
from jax import lax
from jax.experimental import pallas as pl
from jax.experimental.pallas import tpu as pltpu
from jax.sharding import PartitionSpec as P

CHIPS = 4
SLOTS = 2 * CHIPS
TILES = 6
HALF = TILES // 2


def mirror(item):
    return 6 - item + 2 * lax.rem(item, 2)


def gather_item(line, unit):
    slot = lax.div(unit, 2)
    item = jnp.where(slot <= line, 2 * (line - slot), 2 * (slot - line) - 1)
    return (line <= CHIPS - 2) & (slot < 2 * line + 2), item, lax.rem(unit, 2)


def sum_item(line, slot):
    at, ahead = slot - (2 * line + 2), CHIPS - 1 - line
    item = jnp.where(at < ahead, 2 * (line + 1 + at), 2 * (CHIPS - 1 - (at - ahead)) + 1)
    return (line <= CHIPS - 2) & (at >= 0) & (slot < SLOTS), item


def kernel(
    x, wg, wu, wd, y, xg, stash, part, from_left, from_right,
    xv, hv, wgv, wuv, wdv, pst, sst, c_own, c_part, c_up, c_out,
    x_sem, w_sem, wd_sem, first_sem, ag_recv, d2d_recv, d2d_send, send, part_send, part_recv,
    stash_sem, load_sem, sum_send_sem, sum_recv, y_sem, free_sem, up_free,
):
    rows, depth = x.shape
    ft, nt = wg.shape[1] // TILES, wd.shape[1] // TILES
    assert ft == nt
    quarter, half_rows = rows // 4, rows // 2
    me = lax.axis_index("tp")
    z, c = lax.div(me, 2), lax.rem(me, 2)
    partner = me + 1 - 2 * c
    own, other = me, partner
    lines = (z, CHIPS - 1 - z)
    sources = (z - 1, CHIPS - 2 - z)
    targets = (me + 2, me - 2)
    sums = (from_left, from_right)

    def oriented(d, item):
        return item if d == 0 else mirror(item)

    def remote(src, dst, ssem, rsem, device):
        return pltpu.make_async_remote_copy(
            src_ref=src, dst_ref=dst, send_sem=ssem, recv_sem=rsem,
            device_id={"tp": device}, device_id_type=pl.DeviceIdType.MESH,
        )

    def rows_of(half, core):
        return pl.ds(pl.multiple_of((2 * half + core) * quarter, 8), quarter)

    def columns(i, size):
        return pl.ds(pl.multiple_of(i * size, size), size)

    def gather_copy(d, item, half, src):
        return remote(src, xg.at[item, rows_of(half, c)], send.at[d, half], ag_recv.at[item, half], targets[d])

    def start_gather(d, item, half):
        @pl.when(item == own)
        def _():
            gather_copy(d, item, half, x.at[rows_of(half, c)]).start()

        @pl.when(item != own)
        def _():
            gather_copy(d, item, half, xg.at[item, rows_of(half, c)]).start()

    def wait_gathered(item, half):
        gather_copy(0, item, half, xg.at[item, rows_of(half, c)]).wait_recv()

    def pass_on(d, item, half, core):
        at = xg.at[item, rows_of(half, core)]
        return remote(at, at, d2d_send.at[d, half], d2d_recv.at[item, half], partner)

    def gather_service(v):
        for d in range(2):
            valid, item, half = gather_item(sources[d], v - 2)
            item = oriented(d, item)

            @pl.when(valid & (v >= 2))
            def _():
                pass_on(d, item, half, c).wait_send()

            valid, item, half = gather_item(sources[d], v - 1)
            item = oriented(d, item)

            @pl.when(valid)
            def _():
                wait_gathered(item, half)
                pass_on(d, item, half, c).start()

        for d in range(2):
            valid, item, half = gather_item(lines[d], v - 1)

            @pl.when(valid)
            def _():
                gather_copy(d, own, half, xg.at[own, rows_of(half, c)]).wait_send()

            valid, item, half = gather_item(lines[d], v + 1)
            item = oriented(d, item)

            @pl.when(valid)
            def _():
                start_gather(d, item, half)

    def loads(d, item, t, ups):
        pairs = [(stash.at[item, t], c_own.at[d]), (part.at[item, t], c_part.at[d])]
        pairs += [(sums[up].at[item, t], c_up.at[d]) for up in ups]
        return [pltpu.make_async_copy(a, b, load_sem.at[d, i]) for i, (a, b) in enumerate(pairs)]

    def part_copy(item, t):
        return remote(pst.at[t], part.at[item, t], part_send.at[0, t], part_recv.at[item, t], partner)

    def landing(h, t):
        return wgv.at[h * HALF + t, pl.ds(0, rows)]

    def part_last(t):
        return remote(pst.at[t], landing(1 - c, t), part_send.at[0, t], part_recv.at[other, t], partner)

    def part_rest(t):
        at = xv.at[:, columns(t, nt)]
        return remote(at, landing(c, t), part_send.at[1, t], part_recv.at[me, t], partner)

    def sum_sem(d, chip, index, t):
        both = lax.div(index, 2) == chip
        return sum_recv.at[jnp.where(both & (d == 1), SLOTS + lax.rem(index, 2), index), t]

    def sum_copy(d, item, t):
        ends = lax.div(item, 2) == lax.div(targets[d], 2)
        index, device = jnp.where(ends, targets[d], item), jnp.where(ends, item, targets[d])
        return remote(
            c_out.at[d, t], sums[d].at[index, t], sum_send_sem.at[d, t],
            sum_sem(d, lax.div(targets[d], 2), index, t), device,
        )

    def wait_sum(d, index, t):
        at = sums[d].at[index, t]
        remote(at, at, sum_send_sem.at[d, t], sum_sem(d, z, index, t), partner).wait_recv()

    def add(own_ref, others, out):
        step = rows // 11 if rows % 176 == 0 else 16

        @pl.loop(0, rows // step)
        def _(i):
            at = pl.ds(pl.multiple_of(i * step, 16), step)
            total = own_ref[at, :]
            for ref in others:
                total += ref[at, :].astype(jnp.float32)
            out[at, :] = total.astype(jnp.bfloat16)

    def sum_last(d):
        chip = lax.div(targets[d], 2)
        return remote(
            c_out.at[d, HALF - 1], up_landing(c, d), sum_send_sem.at[d, HALF - 1],
            sum_sem(d, chip, targets[d], HALF - 1), 2 * chip + 1,
        )

    def up_landing(h, d):
        return wuv.at[h, pl.ds((2 + d) * rows, rows)]

    def sum_cases(d, slot, act):
        valid, item = sum_item(lines[d], slot)
        item = oriented(d, item)

        @pl.when(valid & (lines[d] == 0))
        def _():
            act(item, ())

        @pl.when(valid & (lines[d] > 0))
        def _():
            act(item, (d,))

    def stored(slot, t):
        @pl.when(slot == 0)
        def _():
            stash_copy(own, t).wait()
            stash_rest(t).wait()

        @pl.when((slot > 0) & (slot < SLOTS - 1))
        def _():
            stash_copy(own, t).wait()
            part_copy(own, t).wait_send()


    def sum_load(slot, t):
        for d in range(2):

            def act(item, ups, d=d):
                part_copy(item, t).wait_recv()
                for up in ups:
                    wait_sum(up, item, t)
                for copy in loads(d, item, t, ups):
                    copy.start()

            sum_cases(d, slot, act)

    def sum_send(slot, t, last=False):
        for d in range(2):

            @pl.when(sum_item(lines[d], slot - 1)[0])
            def _():
                sum_copy(d, own, t).wait_send()

            def act(item, ups, d=d):
                for copy in loads(d, item, t, ups):
                    copy.wait()
                add(c_own.at[d], [c_part.at[d]] + [c_up.at[d] for _ in ups], c_out.at[d, t])
                if last:
                    pl.semaphore_wait(up_free.at[d], 1)
                    sum_last(d).start()
                else:
                    sum_copy(d, item, t).start()

            sum_cases(d, slot, act)

    def item_of(k):
        line = jnp.where(z < 2, z, CHIPS - 1 - z)
        item = jnp.int32(0)
        for i, (a, b) in enumerate(zip((2, 4, 6, 7, 5, 3), (4, 6, 0, 7, 1, 5))):
            item = jnp.where(k == i + 1, jnp.where(line == 0, a, b), item)
        item = jnp.where(z < 2, item, mirror(item))
        return jnp.where(k == 0, own, jnp.where(k == SLOTS - 1, other, item))

    def x_copy(item, half):
        at = pl.ds(half * half_rows, half_rows)
        return pltpu.make_async_copy(xg.at[item, at], xv.at[at], x_sem.at[half])

    def x_load(item, half):
        pass_on(0, item, half, 1 - c).wait_recv()
        x_copy(item, half).start()

    def w_copies(i):
        return [
            pltpu.make_async_copy(w.at[:, columns(i, ft)], v.at[i], w_sem.at[n, i])
            for n, (w, v) in enumerate(((wg, wgv), (wu, wuv)))
        ]

    def wd_copies(pair):
        t, base = lax.rem(pair, HALF), 2 * lax.rem(pair, 2)
        return [
            pltpu.make_async_copy(
                wd.at[:, columns(core * HALF + t, nt)], wdv.at[base + j], wd_sem.at[base + j]
            )
            for j, core in enumerate((c, 1 - c))
        ]

    def stash_copy(item, t):
        return pltpu.make_async_copy(sst.at[t], stash.at[item, t], stash_sem.at[0, t])

    def stash_rest(t):
        return pltpu.make_async_copy(c_own.at[t], stash.at[other, t], stash_sem.at[1, t])

    x_first = pltpu.make_async_copy(x, xv, x_sem.at[0])
    x_first.start()
    for copy in w_copies(0):
        copy.start()
    barrier = pltpu.get_barrier_semaphore()

    def greet(device):
        pl.semaphore_signal(barrier, inc=1, device_id={"tp": device}, device_id_type=pl.DeviceIdType.MESH)

    greet(partner)
    for d in range(2):

        @pl.when(lines[d] <= CHIPS - 2)
        def _():
            greet(targets[d])
            greet(targets[d] + 1 - 2 * c)

    pl.semaphore_wait(barrier, 1 + jnp.where(z > 0, 2, 0) + jnp.where(z < CHIPS - 1, 2, 0))

    def first_copy(n, half):
        at = rows_of(half, 1 - c if n == 0 else c)
        sem = (ag_recv if n == 0 else d2d_recv).at[own, half]
        return remote(x.at[at], xg.at[own, at], first_sem.at[n, half], sem, partner)

    def first_unit(unit):
        for d in range(2):

            @pl.when(lines[d] <= CHIPS - 2)
            def _():
                start_gather(d, 2 * z, unit)

    for half in range(2):
        first_copy(0, half).start()

    @pl.when(c == 0)
    def _():
        first_unit(0)
        first_unit(1)

    for half in range(2):
        first_copy(1, half).start()

    @pl.loop(1, TILES)
    def _(i):
        for copy in w_copies(i):
            copy.start()

    for pair in range(2):
        for copy in wd_copies(jnp.int32(pair)):
            copy.start()
    for half in range(2):
        wait_gathered(other, half)

        @pl.when(c == 1)
        def _():
            first_unit(half)

    x_first.wait()

    spare = pl.ds(0, rows)

    def final_cases(act):
        @pl.when(z == 0)
        def _():
            act((1,))

        @pl.when((z > 0) & (z < CHIPS - 1))
        def _():
            act((0, 1))

        @pl.when(z == CHIPS - 1)
        def _():
            act((0,))

    def own_ref(h, t):
        return c_own.at[t] if h == 0 else sst.at[t]

    def final_copy(h, t, i):
        n, index = h * HALF + t, 2 * z + h
        if i == 0:
            src, dst = stash.at[index, t], own_ref(h, t)
        else:
            src, dst = sums[i - 1].at[index, t], wuv.at[n, pl.ds((i - 1) * rows, rows)]
        sem = (
            w_sem.at[0, n],
            load_sem.at[h, t],
            d2d_send.at[h, t] if t < HALF - 1 else x_sem.at[h],
        )[i]
        return pltpu.make_async_copy(src, dst, sem)

    def up_load(t):
        def act(ups):
            for h in range(2):
                for up in ups:
                    wait_sum(up, 2 * z + h, t)
                    if t < HALF - 1:
                        final_copy(h, t, 1 + up).start()
                    else:

                        @pl.when(c == 0)
                        def _():
                            final_copy(h, t, 1 + up).start()

        final_cases(act)

    def y_copy(h, t):
        return pltpu.make_async_copy(
            hv.at[:, columns(h * HALF + t, nt)], y.at[:, columns(h * HALF + t, nt)], y_sem
        )

    def final_store(t):
        def act(ups):
            for h in range(2):
                n = h * HALF + t
                part_copy(2 * z + h, t).wait_recv()
                final_copy(h, t, 0).wait()

                def total(refs, n=n, h=h):
                    add(own_ref(h, t), [wgv.at[n, spare]] + refs, hv.at[:, columns(n, nt)])

                def loaded(h=h, n=n, total=total):
                    for up in ups:
                        final_copy(h, t, 1 + up).wait()
                    total([wuv.at[n, pl.ds(up * rows, rows)] for up in ups])

                if t < HALF - 1:
                    loaded()
                else:
                    pl.when(c == 0)(loaded)
                    pl.when(c == 1)(lambda h=h, total=total: total([up_landing(h, up) for up in ups]))
                y_copy(h, t).start()

        final_cases(act)

    @pl.loop(0, SLOTS)
    def _(k):
        item, following = item_of(k), item_of(k + 1)

        def gate_up(n, at):
            gate = jnp.dot(xv[at, :], wgv[n], preferred_element_type=jnp.float32)
            up = jnp.dot(xv[at, :], wuv[n], preferred_element_type=jnp.float32)
            hv[at, columns(n, ft)] = (jax.nn.gelu(gate) * up).astype(jnp.bfloat16)

        def prefetch(t):
            for copy in wd_copies(HALF * k + t):
                copy.start()

        @pl.when(k == 0)
        def _():
            @pl.loop(0, HALF)
            def _(i):
                for j in range(2):
                    for copy in w_copies(2 * i + j):
                        copy.wait()
                for j in range(2):
                    gate_up(2 * i + j, pl.ds(0, rows))

        @pl.when(k > 0)
        def _():
            sum_send(k, 0)
            stored(k - 1, 1)
            sum_load(k, 1)
            x_copy(item, 0).wait()

            upper, lower = (pl.ds(half * half_rows, half_rows) for half in range(2))
            for n in range(2):
                gate_up(n, upper)
            gather_service(2 * k)
            sum_send(k, 1)
            for n in range(2, 4):
                gate_up(n, upper)
            x_load(item, 1)
            for n in range(4, TILES):
                gate_up(n, upper)
            stored(k - 1, 2)
            sum_load(k, 2)
            x_copy(item, 1).wait()
            prefetch(0)
            for n in range(2):
                gate_up(n, lower)

            @pl.when(k < SLOTS - 1)
            def _():
                sum_send(k, 2)

            @pl.when((k == SLOTS - 1) & (c == 1))
            def _():
                for d in range(2):

                    @pl.when(sources[d] >= 0)
                    def _():
                        for core in range(2):
                            pl.semaphore_signal(
                                up_free.at[d], inc=1,
                                device_id={"tp": 2 * (z - 1 if d == 0 else z + 1) + core},
                                device_id_type=pl.DeviceIdType.MESH,
                            )

            prefetch(1)
            for n in range(2, TILES):
                gate_up(n, lower)

        def down(pair):
            base = 2 * lax.rem(pair, 2)
            for copy in wd_copies(pair):
                copy.wait()
            return tuple(
                jnp.dot(hv[...], wdv[base + j], preferred_element_type=jnp.float32) for j in range(2)
            )

        @pl.when(k == 0)
        def _():
            @pl.loop(0, HALF)
            def _(t):
                @pl.when(t == 0)
                def _():
                    gather_service(1)

                @pl.when(t == 1)
                def _():
                    x_load(following, 0)

                @pl.when(t == 2)
                def _():
                    stored(0, 0)

                mine, theirs = down(t)
                sst[t] = mine
                c_own[t] = theirs
                stash_copy(own, t).start()
                stash_rest(t).start()

                @pl.when(t == 0)
                def _():
                    prefetch(2)

        @pl.when(k > 0)
        def _():
            def tile_pair(t):
                mine, theirs = down(HALF * k + t)
                sst[t] = mine
                pst[t] = theirs.astype(jnp.bfloat16)

                @pl.when(k < SLOTS - 1)
                def _():
                    stash_copy(item, t).start()
                    part_copy(item, t).start()

            def send_rest(t):
                part_last(t).start()
                add(sst.at[t], [], xv.at[:, columns(t, nt)])
                part_rest(t).start()

            gather_service(2 * k + 1)

            @pl.when(k == SLOTS - 1)
            def _():
                sum_send(k, 2, last=True)
                for n in range(HALF):
                    final_copy(0, n, 0).start()
                up_load(0)
                pl.semaphore_signal(
                    free_sem, inc=1, device_id={"tp": partner}, device_id_type=pl.DeviceIdType.MESH
                )

            tile_pair(0)
            prefetch(2)
            tile_pair(1)

            @pl.when(k < SLOTS - 1)
            def _():
                x_load(following, 0)

            stored(k, 0)
            sum_load(k + 1, 0)

            @pl.when(k == SLOTS - 1)
            def _():
                pl.semaphore_wait(free_sem, 1)
                for t in range(2):
                    send_rest(t)
                    final_copy(1, t, 0).start()
                up_load(1)

            tile_pair(2)

            @pl.when(k == SLOTS - 1)
            def _():
                send_rest(2)
                final_copy(1, 2, 0).start()

    final_store(0)
    final_store(1)
    up_load(2)
    final_store(2)
    for t in range(HALF):
        part_last(t).wait_send()
        part_rest(t).wait_send()
    for d in range(2):

        @pl.when(lines[d] <= CHIPS - 2)
        def _():
            for t in range(HALF):
                sum_copy(d, own, t).wait_send()

    for n in range(2):
        for half in range(2):
            first_copy(n, half).wait_send()
    pltpu.make_async_copy(hv, y, y_sem).wait()


def block(x, w_gate, w_up, w_down):
    rows, depth = x.shape
    width, out = w_gate.shape[1], w_down.shape[1]
    ft, nt = width // TILES, out // TILES
    bf16, f32 = jnp.bfloat16, jnp.float32
    shape = jax.ShapeDtypeStruct
    any_space = pl.BlockSpec(memory_space=pl.ANY)
    dma = pltpu.SemaphoreType.DMA
    results = pl.pallas_call(
        kernel,
        name="mlp_block",
        out_shape=[
            shape((rows, out), bf16),
            shape((SLOTS, rows, depth), bf16),
            shape((SLOTS, HALF, rows, nt), f32),
            shape((SLOTS, HALF, rows, nt), bf16),
            shape((SLOTS, HALF, rows, nt), bf16),
            shape((SLOTS, HALF, rows, nt), bf16),
        ],
        in_specs=[any_space] * 4,
        out_specs=[any_space] * 6,
        scratch_shapes=[
            pltpu.VMEM((rows, depth), bf16),
            pltpu.VMEM((rows, width), bf16),
            pltpu.VMEM((TILES, depth, ft), bf16),
            pltpu.VMEM((TILES, depth, ft), bf16),
            pltpu.VMEM((4, width, nt), bf16),
            pltpu.VMEM((HALF, rows, nt), bf16),
            pltpu.VMEM((HALF, rows, nt), f32),
            pltpu.VMEM((HALF, rows, nt), f32),
            pltpu.VMEM((2, rows, nt), bf16),
            pltpu.VMEM((2, rows, nt), bf16),
            pltpu.VMEM((2, HALF, rows, nt), bf16),
            dma((2,)),
            dma((2, TILES)),
            dma((4,)),
            dma((2, 2)),
            dma((SLOTS, 2)),
            dma((SLOTS, 2)),
            dma((2, 2)),
            dma((2, 2)),
            dma((2, HALF)),
            dma((SLOTS, HALF)),
            dma((2, HALF)),
            dma((2, 3)),
            dma((2, HALF)),
            dma((SLOTS + 2, HALF)),
            dma(()),
            pltpu.SemaphoreType.REGULAR,
            pltpu.SemaphoreType.REGULAR((2,)),
        ],
        compiler_params=pltpu.CompilerParams(
            collective_id=0, has_side_effects=True, vmem_limit_bytes=67_043_328
        ),
    )(x, w_gate, w_up, w_down)
    return results[0]


def solution(mesh):
    return jax.shard_map(
        block,
        mesh=mesh,
        in_specs=(P(("dp", "tp"), None), P(None, "tp"), P(None, "tp"), P("tp", None)),
        out_specs=P(("dp", "tp"), None),
        check_vma=False,
    )
```
